32 devices in a mesh: groups: 2 (over y), ctx: 4 (over x, core), head: 4 (over z).
Axes of the slice: x: 2, y: 2, z: 4, core: 2. Of those that a mesh axis runs over, the one named last changes fastest.
Arguments:
- queries: bfloat16 [384, 64, 128], P(('groups', 'ctx'), 'head'), parts along dimension 0, may hold values from -16 to 16
- prefix_keys: bfloat16 [16384, 8, 128], P(('groups', 'ctx'), 'head'), parts along dimension 0, may hold values from -16 to 16
- prefix_values: bfloat16 [16384, 8, 128], P(('groups', 'ctx'), 'head'), parts along dimension 0, may hold values from -12 to 12
- suffix_keys: bfloat16 [384, 512, 8, 128], P(('groups', 'ctx'), None, 'head'), parts along dimension 0, may hold values from -16 to 16
- suffix_values: bfloat16 [384, 512, 8, 128], P(('groups', 'ctx'), None, 'head'), parts along dimension 0, may hold values from -12 to 12
- lengths: int32 [384], P(('groups', 'ctx')), parts along dimension 0, may hold values from 1 to 512, as said below
Outputs:
- attended: bfloat16 [384, 64, 128], P(('groups', 'ctx'), 'head'), parts along dimension 0
The draws below stay inside these ranges and needn't reach their ends.
There are 2 independent parts, one for each index of `groups`. The reference program is written for one: setup_inputs(seed, part) draws one part's arguments, and reference() takes and returns one part's arrays. A program takes and returns all parts, laid end to end along the dimension named above; each array names one. Nothing has to cross between parts.
Inputs may be any that keep to these rules, and one draw needn't show every extreme that they name: The live slots of a row are its first lengths[r] slots; some row of each part has exactly 512.
All inputs are finite; a program needn't handle non-finite values.
Results may differ from the reference program's by a relative error of at most 0.0025.
Values may be sent and summed in bfloat16 or wider, within the bound.
A program may use at most 128 MiB of HBM per device.

```python
import math
import jax
import jax.numpy as jnp
from jax import lax

Q_HEADS = 64
KV_HEADS = 8
HEAD_DIM = 128
ROWS_DEV = 48
PREFIX_DEV = 2048
SUFFIX = 512
ROWS = 192
PREFIX = 8192
N_CTX = 4


def draw_queries(key, part):
    key_base = jax.random.fold_in(key, 1)
    base_draw = jnp.clip(jax.random.normal(key_base, (ROWS, Q_HEADS, HEAD_DIM), jnp.float32), -5.0, 5.0)
    return base_draw.astype(jnp.bfloat16)


def draw_prefix_keys(key, part):
    key_base = jax.random.fold_in(key, 2)
    base_draw = jnp.clip(2.5 * jax.random.normal(key_base, (PREFIX, KV_HEADS, HEAD_DIM), jnp.float32), -15.0, 15.0)
    return base_draw.astype(jnp.bfloat16)


def draw_lengths(key, part):
    key_level, key_raw, key_long = jax.random.split(jax.random.fold_in(key, 5), 3)
    block_count = ROWS // ROWS_DEV
    levels = jax.random.randint(key_level, (block_count,), 1, 9)
    ceiling = jnp.repeat(SUFFIX * levels // 8, ROWS_DEV, total_repeat_length=ROWS)
    raw_draw = jax.random.randint(key_raw, (ROWS,), 0, SUFFIX)
    result = 1 + raw_draw % ceiling
    longest = jax.random.randint(key_long, (), 0, ROWS)
    result = result.at[longest].set(SUFFIX)
    return result.astype(jnp.int32)


def block_levels(rng, shape, cuts, low, high):
    loudness = 1.0
    for position, shards_of in cuts:
        draws = jax.random.uniform(jax.random.fold_in(jax.random.fold_in(rng, 6), position), (shards_of,), jnp.float32, low / len(cuts), high / len(cuts))
        loudness = loudness * jnp.repeat(jnp.exp(draws), shape[position] // shards_of).reshape((-1,) + (1,) * (len(shape) - 1 - position))
    return loudness


def normal_values(stream_key, dims, deviation, limit, cuts=(), kind=jnp.bfloat16):
    array = jax.random.normal(stream_key, dims, jnp.float32) * deviation
    if len(cuts) > 0:
        array = block_levels(stream_key, dims, cuts, -0.22, 0.18) * array
    return jnp.clip(array, min=-limit, max=limit).astype(kind)


def setup_inputs(seed: int = 0, part: int = 0) -> dict:
    streams_of = jax.random.split(jax.random.key(seed), 7)
    part_splits = jax.random.split(jax.random.fold_in(streams_of[6], part), 7)
    queries = draw_queries(jax.random.fold_in(jax.random.fold_in(streams_of[6], part), 71), part)
    prefix_keys = draw_prefix_keys(jax.random.fold_in(jax.random.fold_in(streams_of[6], part), 71), part)
    prefix_values = normal_values(part_splits[2], (PREFIX, KV_HEADS, HEAD_DIM), 2.0, 12.0, ((0, 4), (1, 4)))
    suffix_keys = normal_values(part_splits[3], (ROWS, SUFFIX, KV_HEADS, HEAD_DIM), 4.0, 16.0, ((0, 4), (2, 4)))
    suffix_values = normal_values(part_splits[4], (ROWS, SUFFIX, KV_HEADS, HEAD_DIM), 2.0, 12.0, ((0, 4), (2, 4)))
    lengths = draw_lengths(jax.random.fold_in(jax.random.fold_in(streams_of[6], part), 71), part)
    return {"queries": queries, "prefix_keys": prefix_keys, "prefix_values": prefix_values, "suffix_keys": suffix_keys, "suffix_values": suffix_values, "lengths": lengths}


def reference(queries, prefix_keys, prefix_values, suffix_keys, suffix_values, lengths):
    rows, heads, head_width = queries.shape
    kv_count = prefix_keys.shape[1]
    group_size = heads // kv_count
    span = suffix_keys.shape[1]
    scaling = head_width ** -0.5
    keys_wide = prefix_keys.astype(jnp.float32)
    values_wide = prefix_values.astype(jnp.float32).reshape(N_CTX, PREFIX_DEV, kv_count, head_width)
    positions = jnp.arange(span, dtype=jnp.int32)
    block_rows = math.gcd(rows, 8)
    count_blocks = rows // block_rows

    def one_block(pieces):
        query_block, keys_block, values_block, length_block = pieces
        grouped = query_block.astype(jnp.float32).reshape(block_rows, kv_count, group_size, head_width)
        prefix_part = jnp.einsum("rkgd,pkd->rkgp", grouped, keys_wide, precision=lax.Precision.HIGHEST) * scaling
        prefix_part = prefix_part.reshape(block_rows, kv_count, group_size, N_CTX, PREFIX_DEV)
        suffix_part = jnp.einsum("rkgd,rskd->rkgs", grouped, keys_block.astype(jnp.float32), precision=lax.Precision.HIGHEST) * scaling
        live_mask = (positions[None, :] < length_block[:, None])[:, None, None, :]
        block_top = jnp.max(prefix_part, axis=-1)
        row_top = jnp.maximum(jnp.max(block_top, axis=-1), jnp.max(jnp.where(live_mask, suffix_part, -jnp.inf), axis=-1))
        prefix_weights = jnp.exp(prefix_part - block_top[..., None]).astype(jnp.bfloat16)
        block_scale = jnp.exp(block_top - row_top[..., None])
        suffix_weights = jnp.where(live_mask, jnp.exp(suffix_part - row_top[..., None]), 0.0).astype(jnp.bfloat16)
        prefix_float = prefix_weights.astype(jnp.float32)
        suffix_float = suffix_weights.astype(jnp.float32)
        weight_sum = jnp.sum(jnp.sum(prefix_float, axis=-1) * block_scale, axis=-1) + jnp.sum(suffix_float, axis=-1)
        partial_accum = jnp.einsum("rkgcp,cpkd->rkgcd", prefix_float, values_wide, precision=lax.Precision.HIGHEST)
        accumulated = jnp.sum(partial_accum * block_scale[..., None], axis=-2)
        accumulated = accumulated + jnp.einsum("rkgs,rskd->rkgd", suffix_float, values_block.astype(jnp.float32), precision=lax.Precision.HIGHEST)
        result = (accumulated / weight_sum[..., None]).astype(jnp.bfloat16)
        return result.reshape(block_rows, heads, head_width)

    stacked = lax.map(one_block, (
        queries.reshape(count_blocks, block_rows, heads, head_width),
        suffix_keys.reshape(count_blocks, block_rows, span, kv_count, head_width),
        suffix_values.reshape(count_blocks, block_rows, span, kv_count, head_width),
        lengths.reshape(count_blocks, block_rows)))
    return stacked.reshape(rows, heads, head_width)
```

```python
import functools
import math

import jax
import jax.numpy as jnp
from jax import lax
from jax.experimental import pallas as pl
from jax.experimental.pallas import tpu as pltpu
from jax.sharding import PartitionSpec as P

F32 = jnp.float32
BF16 = jnp.bfloat16
MASKED = -1e30
LANES = 128


def dot_t(a, b):
    return lax.dot_general(a, b, (((1,), (1,)), ((), ())), preferred_element_type=F32)


def kernel(
    n_ctx, tile_rows, first_tiles,
    len_ref, q_hbm, pk_hbm, pv_hbm, sk_hbm, sv_hbm, out_ref,
    q_raw, qk, k_raw, v_raw, k_cut, v_cut, wide, sk, sv,
    part_acc, part_stat, got_acc, got_stat,
    own_acc, own_top, own_sum, suf_acc, suf_top, suf_sum,
    q_sem, kv_sem, suf_sem, q_send, q_recv, kv_send, kv_recv, p_send, p_recv,
):
    rows, heads, width = q_hbm.shape
    kv = k_cut.shape[1]
    group = heads // kv
    flat = rows * group
    pair = 2 if n_ctx % 2 == 0 else 1
    chips = n_ctx // pair
    blocks = pair
    factor = width ** (-0.5) * math.log2(math.e)
    tiles = rows // tile_rows
    slots = sk.shape[1]
    me = lax.axis_index("ctx")
    chip, core = me // pair, me % pair

    def device(chip_at, core_at):
        return {"ctx": chip_at * pair + core_at}

    def remote(src, dst, send, recv, target):
        return pltpu.make_async_remote_copy(
            src_ref=src, dst_ref=dst, send_sem=send, recv_sem=recv,
            device_id=target, device_id_type=pl.DeviceIdType.MESH,
        )

    q_copy = pltpu.make_async_copy(q_hbm, q_raw.at[0], q_sem)
    q_copy.start()
    kv_copies = [
        pltpu.make_async_copy(pk_hbm, k_raw.at[0], kv_sem.at[0]),
        pltpu.make_async_copy(pv_hbm, v_raw.at[0], kv_sem.at[1]),
    ]
    for copy in kv_copies:
        copy.start()

    def suffix_copies(tile):
        span = pl.ds(tile * tile_rows, tile_rows)
        return (
            pltpu.make_async_copy(sk_hbm.at[span], sk.at[span], suf_sem.at[tile, 0]),
            pltpu.make_async_copy(sv_hbm.at[span], sv.at[span], suf_sem.at[tile, 1]),
        )

    partners = [device(lax.rem(chip + t, chips), core) for t in range(1, chips)]
    backs = [device(lax.rem(chip - t + chips, chips), core) for t in range(1, chips)]
    twin = device(chip, pair - 1 - core)
    greeted = partners + ([twin] if pair == 2 else [])
    if greeted:
        barrier = pltpu.get_barrier_semaphore()
        for target in greeted:
            pl.semaphore_signal(
                barrier, inc=1, device_id=target, device_id_type=pl.DeviceIdType.MESH
            )
        pl.semaphore_wait(barrier, len(greeted))

    q_sends = [
        remote(q_hbm, q_raw.at[t + 1], q_send.at[t], q_recv.at[t], partners[t])
        for t in range(chips - 1)
    ]
    for copy in q_sends:
        copy.start()
    kv_sends = []
    if pair == 2:
        kv_sends = [
            remote(pk_hbm, k_raw.at[1], kv_send.at[0], kv_recv.at[0], twin),
            remote(pv_hbm, v_raw.at[1], kv_send.at[1], kv_recv.at[1], twin),
        ]
        for copy in kv_sends:
            copy.start()

    def start_tile(tile, carry):
        for copy in suffix_copies(tile):
            copy.start()
        return carry

    lax.fori_loop(0, tiles, start_tile, 0)

    def split_queries(slot):
        wide_q = q_raw[slot].astype(F32).reshape(rows, kv, group, width)
        for k in range(kv):
            qk[slot, k] = wide_q[:, k].reshape(flat, width).astype(BF16)

    span = k_cut.shape[2]
    piece = wide.shape[1]
    pieces = span * kv // piece

    def split_block(block):
        def step(i, carry):
            at = pl.ds(pl.multiple_of(i * piece, piece), piece)
            to = pl.ds(pl.multiple_of(i * (piece // kv), piece // kv), piece // kv)
            wide[0] = k_raw[block, at, :].astype(F32)
            wide[1] = v_raw[block, at, :].astype(F32)
            for k in range(kv):
                rows_k = pl.ds(k, piece // kv, stride=kv) if kv > 1 else pl.ds(0, piece)
                k_cut[block, k, to, :] = wide[0, rows_k, :].astype(BF16)
                v_cut[block, k, to, 0:width] = wide[1, rows_k, :].astype(BF16)
                v_cut[block, k, to, width : 2 * width] = jnp.ones((piece // kv, width), BF16)
            return carry

        lax.fori_loop(0, pieces, step, 0)

    step_rows = LANES

    def block_terms(slot, k, block, at):
        scores = dot_t(qk[slot, k, at, :], k_cut[block, k]) * factor
        top = jnp.max(scores, axis=1, keepdims=True)
        weights = jnp.exp2(scores - top).astype(BF16)
        both = jnp.dot(weights, v_cut[block, k], preferred_element_type=F32)
        return top, both[:, :width], both[:, width:]

    def merge(one, two):
        top = jnp.maximum(one[0], two[0])
        a, b = jnp.exp2(one[0] - top), jnp.exp2(two[0] - top)
        return top, one[1] * a + two[1] * b, one[2] * a + two[2] * b

    chunks = flat // step_rows

    def own_block(block):
        def step(k, carry):
            for c in range(chunks):
                at = pl.ds(c * step_rows, step_rows)
                terms = block_terms(0, k, block, at)
                if block > 0:
                    terms = merge(terms, (own_top[k, at, :], own_acc[k, at, :], own_sum[k, at, :]))
                own_top[k, at, :] = jnp.broadcast_to(terms[0], (step_rows, width))
                own_acc[k, at, :] = terms[1]
                own_sum[k, at, :] = terms[2]
            return carry

        lax.fori_loop(0, kv, step, 0)

    diagonal = lax.broadcasted_iota(jnp.int32, (step_rows, LANES), 0) == lax.broadcasted_iota(
        jnp.int32, (step_rows, LANES), 1
    )

    def partial_copies(t, k):
        return (
            remote(part_acc.at[t, k], got_acc.at[t, k], p_send.at[t, k, 0], p_recv.at[t, k, 0], backs[t]),
            remote(part_stat.at[t, k], got_stat.at[t, k], p_send.at[t, k, 1], p_recv.at[t, k, 1], backs[t]),
        )

    def remote_rows(t):
        for k in range(kv):
            stat = []
            for c in range(chunks):
                at = pl.ds(c * step_rows, step_rows)
                terms = block_terms(t + 1, k, 0, at)
                for block in range(1, blocks):
                    terms = merge(terms, block_terms(t + 1, k, block, at))
                part_acc[t, k, at, :] = terms[1]
                top_wide = jnp.broadcast_to(terms[0], (step_rows, LANES))
                for i, x in enumerate((top_wide, terms[2])):
                    row = 2 * c + i
                    part_stat[t, k, row : row + 1, :] = jnp.sum(
                        jnp.where(diagonal, x, 0.0), axis=0, keepdims=True
                    )
            for copy in partial_copies(t, k):
                copy.start()

    column = lax.broadcasted_iota(jnp.int32, (heads, slots), 1)
    same_head = column % kv == lax.broadcasted_iota(jnp.int32, (heads, slots), 0) // group

    def suffix_tile(tile, carry):
        for copy in suffix_copies(tile):
            copy.wait()
        for i in range(tile_rows):
            r = tile * tile_rows + i
            live = same_head & (column < len_ref[r] * kv)
            scores = jnp.where(live, dot_t(q_raw[0, r], sk[r]) * factor, MASKED)
            top = jnp.max(scores, axis=1, keepdims=True)
            weights = jnp.exp2(scores - top).astype(BF16)
            total = jnp.sum(weights.astype(F32), axis=1, keepdims=True)
            acc = jnp.dot(weights, sv[r], preferred_element_type=F32)
            top = jnp.broadcast_to(top, (heads, width))
            total = jnp.broadcast_to(total, (heads, width))
            to = pl.ds(pl.multiple_of(r * group, group), group)
            for k in range(kv):
                part = slice(k * group, (k + 1) * group)
                suf_acc[k, to, :] = acc[part]
                suf_top[k, to, :] = top[part]
                suf_sum[k, to, :] = total[part]
        return carry

    q_copy.wait()
    split_queries(0)
    for copy in kv_copies:
        copy.wait()
    split_block(0)
    own_block(0)
    lax.fori_loop(0, first_tiles, suffix_tile, 0)
    for copy in kv_sends:
        copy.wait_recv()
    for block in range(1, blocks):
        split_block(block)
    for t in range(chips - 1):
        q_sends[t].wait_recv()
        split_queries(t + 1)
        remote_rows(t)
    for block in range(1, blocks):
        own_block(block)
    lax.fori_loop(first_tiles, tiles, suffix_tile, 0)

    for k in range(kv):
        for t in range(chips - 1):
            for copy in partial_copies(t, k):
                copy.wait_recv()
    per = step_rows // group
    for c in range(chunks):
        at = pl.ds(c * step_rows, step_rows)
        done = []
        for k in range(kv):
            terms = merge(
                (own_top[k, at, :], own_acc[k, at, :], own_sum[k, at, :]),
                (suf_top[k, at, :], suf_acc[k, at, :], suf_sum[k, at, :]),
            )
            for t in range(chips - 1):
                stats = []
                for i in range(2):
                    row = jnp.broadcast_to(
                        got_stat[t, k, 2 * c + i : 2 * c + i + 1, :], (step_rows, LANES)
                    )
                    stats.append(jnp.sum(jnp.where(diagonal, row, 0.0), axis=1, keepdims=True))
                terms = merge(terms, (stats[0], got_acc[t, k, at, :], stats[1]))
            done.append((terms[1] / terms[2]).reshape(per, 1, group, width))
        joined = jnp.concatenate(done, axis=1).reshape(per, heads, width)
        out_ref[c * per : (c + 1) * per] = joined.astype(BF16)
    for copy in q_sends + kv_sends:
        copy.wait_send()
    for t in range(chips - 1):
        for k in range(kv):
            for copy in partial_copies(t, k):
                copy.wait_send()


def shards(n_ctx, queries, prefix_keys, prefix_values, suffix_keys, suffix_values, lengths):
    rows, heads, width = queries.shape
    positions, kv, _ = prefix_keys.shape
    slots = suffix_keys.shape[1] * kv
    flat = rows * (heads // kv)
    pair = 2 if n_ctx % 2 == 0 else 1
    others = max(1, n_ctx // pair - 1)
    tile_rows = math.gcd(rows, 4)
    tiles = rows // tile_rows
    first_tiles = tiles // 3
    stat_rows = -(-2 * (flat // LANES) // 8) * 8
    piece = math.gcd(positions * kv, 1024)
    anywhere = pl.BlockSpec(memory_space=pl.ANY)
    vmem = pltpu.VMEM
    dma = pltpu.SemaphoreType.DMA
    call = pl.pallas_call(
        functools.partial(kernel, n_ctx, tile_rows, first_tiles),
        out_shape=jax.ShapeDtypeStruct((rows, heads, width), BF16),
        in_specs=[pl.BlockSpec(memory_space=pltpu.SMEM)] + [anywhere] * 5,
        out_specs=pl.BlockSpec(memory_space=vmem),
        scratch_shapes=[
            vmem((1 + others, rows, heads, width), BF16),
            vmem((1 + others, kv, flat, width), BF16),
            vmem((pair, positions * kv, width), BF16),
            vmem((pair, positions * kv, width), BF16),
            vmem((pair, kv, positions, width), BF16),
            vmem((pair, kv, positions, 2 * width), BF16),
            vmem((2, piece, width), F32),
            vmem((rows, slots, width), BF16),
            vmem((rows, slots, width), BF16),
            vmem((others, kv, flat, width), F32),
            vmem((others, kv, stat_rows, LANES), F32),
            vmem((others, kv, flat, width), F32),
            vmem((others, kv, stat_rows, LANES), F32),
        ]
        + [vmem((kv, flat, width), F32)] * 6
        + [
            dma,
            dma((2,)),
            dma((tiles, 2)),
            dma((others,)),
            dma((others,)),
            dma((2,)),
            dma((2,)),
            dma((others, kv, 2)),
            dma((others, kv, 2)),
        ],
        compiler_params=pltpu.CompilerParams(
            collective_id=0, has_side_effects=True, vmem_limit_bytes=62 * 1024 * 1024
        ),
    )
    return call(
        lengths,
        queries,
        prefix_keys.reshape(positions * kv, width),
        prefix_values.reshape(positions * kv, width),
        suffix_keys.reshape(rows, slots, width),
        suffix_values.reshape(rows, slots, width),
    )


def solution(mesh):
    placed = (
        P(("groups", "ctx"), "head", None),
        P(("groups", "ctx"), "head", None),
        P(("groups", "ctx"), "head", None),
        P(("groups", "ctx"), None, "head", None),
        P(("groups", "ctx"), None, "head", None),
        P(("groups", "ctx")),
    )
    return jax.shard_map(
        functools.partial(shards, mesh.shape["ctx"]),
        mesh=mesh,
        in_specs=placed,
        out_specs=P(("groups", "ctx"), "head", None),
        check_vma=False,
    )
```

```python
import functools
import math

import jax
import jax.numpy as jnp
from jax import lax
from jax.experimental import pallas as pl
from jax.experimental.pallas import tpu as pltpu
from jax.sharding import PartitionSpec as P

F32 = jnp.float32
BF16 = jnp.bfloat16
MASKED = -1e30
LANES = 128


def dot_t(a, b):
    return lax.dot_general(a, b, (((1,), (1,)), ((), ())), preferred_element_type=F32)


def kernel(
    n_ctx, tile_rows, first_tiles,
    len_ref, q_hbm, pk_hbm, pv_hbm, sk_hbm, sv_hbm, out_ref,
    q_raw, q_far, qk, k_raw, v_raw, k_cut, v_cut, wide, sk, sv,
    part_acc, part_stat, got_acc, got_stat,
    own_acc, own_top, own_sum, suf_acc, suf_top, suf_sum,
    q_sem, kv_sem, suf_sem, q_send, q_recv, kv_send, kv_recv, p_send, p_recv,
):
    rows, heads, width = q_hbm.shape
    kv = k_cut.shape[1]
    group = heads // kv
    flat = rows * group
    pair = 2 if n_ctx % 2 == 0 else 1
    chips = n_ctx // pair
    blocks = pair
    factor = width ** (-0.5) * math.log2(math.e)
    tiles = rows // tile_rows
    slots = sk.shape[1]
    me = lax.axis_index("ctx")
    chip, core = me // pair, me % pair

    def device(chip_at, core_at):
        return {"ctx": chip_at * pair + core_at}

    def remote(src, dst, send, recv, target):
        return pltpu.make_async_remote_copy(
            src_ref=src, dst_ref=dst, send_sem=send, recv_sem=recv,
            device_id=target, device_id_type=pl.DeviceIdType.MESH,
        )

    q_copy = pltpu.make_async_copy(q_hbm, q_raw.at[0], q_sem)
    q_copy.start()
    kv_copies = [
        pltpu.make_async_copy(pk_hbm, k_raw.at[0], kv_sem.at[0]),
        pltpu.make_async_copy(pv_hbm, v_raw.at[0], kv_sem.at[1]),
    ]
    for copy in kv_copies:
        copy.start()

    def suffix_copies(tile):
        span = pl.ds(tile * tile_rows, tile_rows)
        return (
            pltpu.make_async_copy(sk_hbm.at[span], sk.at[span], suf_sem.at[tile, 0]),
            pltpu.make_async_copy(sv_hbm.at[span], sv.at[span], suf_sem.at[tile, 1]),
        )

    partners = [device(lax.rem(chip + t, chips), core) for t in range(1, chips)]
    backs = [device(lax.rem(chip - t + chips, chips), core) for t in range(1, chips)]
    twin = device(chip, pair - 1 - core)
    greeted = partners + ([twin] if pair == 2 else [])
    if greeted:
        barrier = pltpu.get_barrier_semaphore()
        for target in greeted:
            pl.semaphore_signal(
                barrier, inc=1, device_id=target, device_id_type=pl.DeviceIdType.MESH
            )
        pl.semaphore_wait(barrier, len(greeted))

    q_sends = [
        [
            remote(
                q_hbm.at[:, k * group : (k + 1) * group, :], q_far.at[t, k],
                q_send.at[t, k], q_recv.at[t, k], partners[t],
            )
            for k in range(kv)
        ]
        for t in range(chips - 1)
    ]
    for k in range(kv):
        for copies in q_sends:
            copies[k].start()
    kv_sends = []
    if pair == 2:
        kv_sends = [
            remote(pk_hbm, k_raw.at[1], kv_send.at[0], kv_recv.at[0], twin),
            remote(pv_hbm, v_raw.at[1], kv_send.at[1], kv_recv.at[1], twin),
        ]
        for copy in kv_sends:
            copy.start()

    def start_tile(tile, carry):
        for copy in suffix_copies(tile):
            copy.start()
        return carry

    lax.fori_loop(0, tiles, start_tile, 0)

    def split_queries():
        wide_q = q_raw[0].astype(F32).reshape(rows, kv, group, width)
        for k in range(kv):
            qk[0, k] = wide_q[:, k].reshape(flat, width).astype(BF16)

    span = k_cut.shape[2]
    piece = wide.shape[1]
    pieces = span * kv // piece

    def split_block(block):
        def step(i, carry):
            at = pl.ds(pl.multiple_of(i * piece, piece), piece)
            to = pl.ds(pl.multiple_of(i * (piece // kv), piece // kv), piece // kv)
            wide[0] = k_raw[block, at, :].astype(F32)
            wide[1] = v_raw[block, at, :].astype(F32)
            for k in range(kv):
                rows_k = pl.ds(k, piece // kv, stride=kv) if kv > 1 else pl.ds(0, piece)
                k_cut[block, k, to, :] = wide[0, rows_k, :].astype(BF16)
                v_cut[block, k, to, 0:width] = wide[1, rows_k, :].astype(BF16)
                v_cut[block, k, to, width : 2 * width] = jnp.ones((piece // kv, width), BF16)
            return carry

        lax.fori_loop(0, pieces, step, 0)

    step_rows = LANES

    def block_terms(slot, k, block, at):
        scores = dot_t(qk[slot, k, at, :], k_cut[block, k]) * factor
        top = jnp.max(scores, axis=1, keepdims=True)
        weights = jnp.exp2(scores - top).astype(BF16)
        both = jnp.dot(weights, v_cut[block, k], preferred_element_type=F32)
        return top, both[:, :width], both[:, width:]

    def merge(one, two):
        top = jnp.maximum(one[0], two[0])
        a, b = jnp.exp2(one[0] - top), jnp.exp2(two[0] - top)
        return top, one[1] * a + two[1] * b, one[2] * a + two[2] * b

    chunks = flat // step_rows

    def own_block(block):
        def step(k, carry):
            for c in range(chunks):
                at = pl.ds(c * step_rows, step_rows)
                terms = block_terms(0, k, block, at)
                if block > 0:
                    terms = merge(terms, (own_top[k, at, :], own_acc[k, at, :], own_sum[k, at, :]))
                own_top[k, at, :] = jnp.broadcast_to(terms[0], (step_rows, width))
                own_acc[k, at, :] = terms[1]
                own_sum[k, at, :] = terms[2]
            return carry

        lax.fori_loop(0, kv, step, 0)

    diagonal = lax.broadcasted_iota(jnp.int32, (step_rows, LANES), 0) == lax.broadcasted_iota(
        jnp.int32, (step_rows, LANES), 1
    )

    def partial_copy(t, k, c):
        if c == chunks:
            src, dst = part_stat.at[t, k], got_stat.at[t, k]
        else:
            at = pl.ds(c * step_rows, step_rows)
            src, dst = part_acc.at[t, k, at], got_acc.at[t, k, at]
        return remote(src, dst, p_send.at[t, k, c], p_recv.at[t, k, c], backs[t])

    def partial_copies(t, k):
        return [partial_copy(t, k, c) for c in range(chunks + 1)]

    def remote_rows(t):
        for k in range(kv):
            q_sends[t][k].wait_recv()
            qk[t + 1, k] = q_far[t, k].astype(F32).reshape(flat, width).astype(BF16)
            for c in range(chunks):
                at = pl.ds(c * step_rows, step_rows)
                terms = block_terms(t + 1, k, 0, at)
                for block in range(1, blocks):
                    terms = merge(terms, block_terms(t + 1, k, block, at))
                part_acc[t, k, at, :] = terms[1]
                top_wide = jnp.broadcast_to(terms[0], (step_rows, LANES))
                for i, x in enumerate((top_wide, terms[2])):
                    row = 2 * c + i
                    part_stat[t, k, row : row + 1, :] = jnp.sum(
                        jnp.where(diagonal, x, 0.0), axis=0, keepdims=True
                    )
                partial_copy(t, k, c).start()
            partial_copy(t, k, chunks).start()

    column = lax.broadcasted_iota(jnp.int32, (heads, slots), 1)
    same_head = column % kv == lax.broadcasted_iota(jnp.int32, (heads, slots), 0) // group

    def suffix_tile(tile, carry):
        for copy in suffix_copies(tile):
            copy.wait()
        for i in range(tile_rows):
            r = tile * tile_rows + i
            live = same_head & (column < len_ref[r] * kv)
            scores = jnp.where(live, dot_t(q_raw[0, r], sk[r]) * factor, MASKED)
            top = jnp.max(scores, axis=1, keepdims=True)
            weights = jnp.exp2(scores - top).astype(BF16)
            total = jnp.sum(weights.astype(F32), axis=1, keepdims=True)
            acc = jnp.dot(weights, sv[r], preferred_element_type=F32)
            top = jnp.broadcast_to(top, (heads, width))
            total = jnp.broadcast_to(total, (heads, width))
            to = pl.ds(pl.multiple_of(r * group, group), group)
            for k in range(kv):
                part = slice(k * group, (k + 1) * group)
                suf_acc[k, to, :] = acc[part]
                suf_top[k, to, :] = top[part]
                suf_sum[k, to, :] = total[part]
        return carry

    q_copy.wait()
    split_queries()
    for copy in kv_copies:
        copy.wait()
    split_block(0)
    own_block(0)
    lax.fori_loop(0, first_tiles, suffix_tile, 0)
    for copy in kv_sends:
        copy.wait_recv()
    for block in range(1, blocks):
        split_block(block)
    for t in range(chips - 1):
        remote_rows(t)
    for block in range(1, blocks):
        own_block(block)
    lax.fori_loop(first_tiles, tiles, suffix_tile, 0)

    for k in range(kv):
        for t in range(chips - 1):
            for copy in partial_copies(t, k):
                copy.wait_recv()
    per = step_rows // group
    for c in range(chunks):
        at = pl.ds(c * step_rows, step_rows)
        done = []
        for k in range(kv):
            terms = merge(
                (own_top[k, at, :], own_acc[k, at, :], own_sum[k, at, :]),
                (suf_top[k, at, :], suf_acc[k, at, :], suf_sum[k, at, :]),
            )
            for t in range(chips - 1):
                stats = []
                for i in range(2):
                    row = jnp.broadcast_to(
                        got_stat[t, k, 2 * c + i : 2 * c + i + 1, :], (step_rows, LANES)
                    )
                    stats.append(jnp.sum(jnp.where(diagonal, row, 0.0), axis=1, keepdims=True))
                terms = merge(terms, (stats[0], got_acc[t, k, at, :], stats[1]))
            done.append((terms[1] / terms[2]).reshape(per, 1, group, width))
        joined = jnp.concatenate(done, axis=1).reshape(per, heads, width)
        out_ref[c * per : (c + 1) * per] = joined.astype(BF16)
    for copy in sum(q_sends, []) + kv_sends:
        copy.wait_send()
    for t in range(chips - 1):
        for k in range(kv):
            for copy in partial_copies(t, k):
                copy.wait_send()


def shards(n_ctx, queries, prefix_keys, prefix_values, suffix_keys, suffix_values, lengths):
    rows, heads, width = queries.shape
    positions, kv, _ = prefix_keys.shape
    slots = suffix_keys.shape[1] * kv
    flat = rows * (heads // kv)
    pair = 2 if n_ctx % 2 == 0 else 1
    others = max(1, n_ctx // pair - 1)
    tile_rows = math.gcd(rows, 4)
    tiles = rows // tile_rows
    first_tiles = tiles // 6
    stat_rows = -(-2 * (flat // LANES) // 8) * 8
    piece = math.gcd(positions * kv, 1024)
    anywhere = pl.BlockSpec(memory_space=pl.ANY)
    vmem = pltpu.VMEM
    dma = pltpu.SemaphoreType.DMA
    call = pl.pallas_call(
        functools.partial(kernel, n_ctx, tile_rows, first_tiles),
        out_shape=jax.ShapeDtypeStruct((rows, heads, width), BF16),
        in_specs=[pl.BlockSpec(memory_space=pltpu.SMEM)] + [anywhere] * 5,
        out_specs=pl.BlockSpec(memory_space=vmem),
        scratch_shapes=[
            vmem((1, rows, heads, width), BF16),
            vmem((others, kv, rows, heads // kv, width), BF16),
            vmem((1 + others, kv, flat, width), BF16),
            vmem((pair, positions * kv, width), BF16),
            vmem((pair, positions * kv, width), BF16),
            vmem((pair, kv, positions, width), BF16),
            vmem((pair, kv, positions, 2 * width), BF16),
            vmem((2, piece, width), F32),
            vmem((rows, slots, width), BF16),
            vmem((rows, slots, width), BF16),
            vmem((others, kv, flat, width), F32),
            vmem((others, kv, stat_rows, LANES), F32),
            vmem((others, kv, flat, width), F32),
            vmem((others, kv, stat_rows, LANES), F32),
        ]
        + [vmem((kv, flat, width), F32)] * 6
        + [
            dma,
            dma((2,)),
            dma((tiles, 2)),
            dma((others, kv)),
            dma((others, kv)),
            dma((2,)),
            dma((2,)),
            dma((others, kv, flat // LANES + 1)),
            dma((others, kv, flat // LANES + 1)),
        ],
        compiler_params=pltpu.CompilerParams(
            collective_id=0, has_side_effects=True, vmem_limit_bytes=62 * 1024 * 1024
        ),
    )
    return call(
        lengths,
        queries,
        prefix_keys.reshape(positions * kv, width),
        prefix_values.reshape(positions * kv, width),
        suffix_keys.reshape(rows, slots, width),
        suffix_values.reshape(rows, slots, width),
    )


def solution(mesh):
    placed = (
        P(("groups", "ctx"), "head", None),
        P(("groups", "ctx"), "head", None),
        P(("groups", "ctx"), "head", None),
        P(("groups", "ctx"), None, "head", None),
        P(("groups", "ctx"), None, "head", None),
        P(("groups", "ctx")),
    )
    return jax.shard_map(
        functools.partial(shards, mesh.shape["ctx"]),
        mesh=mesh,
        in_specs=placed,
        out_specs=P(("groups", "ctx"), "head", None),
        check_vma=False,
    )
```
